32 devices in a mesh: row: 4 (over y, core), col: 8 (over z, x).
Axes of the slice: x: 2, y: 2, z: 4, core: 2. Of those that a mesh axis runs over, the one named last changes fastest.
Arguments:
- templates: float32 [96, 3, 1024], P(('row', 'col')), may hold values from -600 to 600
Outputs:
- similar: float32 [96, 96], P(('row', 'col'))
The draws below stay inside these ranges and needn't reach their ends.
All inputs are finite; a program needn't handle non-finite values.
Results may differ from the reference program's by a relative error of at most 0.0012.
Values may be sent and summed in bfloat16 or wider, within the bound.
A program may use at most 128 MiB of HBM per device.

```python
import math
import jax
import jax.numpy as jnp
from jax import lax

COMP = 3
SAMPLES = 1024
LAGS = 512
NFFT = 1280
NT = 96


def draw_templates(key, part):
    subkeys = jax.random.split(key, 6)
    noise_part = jnp.clip(jax.random.normal(subkeys[0], (NT, COMP, SAMPLES), jnp.float32), -6.0, 6.0)
    weight = jax.random.uniform(subkeys[4], (NT, 1, 1), jnp.float32, 0.0, 1.5)
    scales = jnp.exp(jax.random.uniform(subkeys[5], (NT, COMP, 1), jnp.float32, 0.0, jnp.log(10.0)))
    clusters = jnp.clip(jax.random.normal(subkeys[1], (8, COMP, SAMPLES), jnp.float32), -6.0, 6.0)
    member = jax.random.randint(subkeys[2], (NT,), 0, 8)
    shifts = jax.random.randint(subkeys[3], (NT,), -(LAGS // 4), LAGS // 4 + 1)
    source_idx = (jnp.arange(SAMPLES, dtype=jnp.int32)[None, :] - shifts[:, None]) % SAMPLES
    chosen = clusters[member]
    shifted = jnp.take_along_axis(chosen, jnp.broadcast_to(source_idx[:, None, :], (NT, COMP, SAMPLES)), axis=2)
    return ((weight * shifted + noise_part) * scales).astype(jnp.float32)


def setup_inputs(seed: int = 0) -> dict:
    splits = jax.random.split(jax.random.key(seed), 2)
    templates = draw_templates(jax.random.fold_in(splits[1], 71), 0)
    return {"templates": templates}


def normalize(templates):
    scaling = lax.rsqrt(lax.optimization_barrier(jnp.mean(templates * templates, axis=2, keepdims=True)) + 1e-06) / math.sqrt(templates.shape[2])
    return (templates * scaling).astype(jnp.bfloat16)

def forward_table(samples, transform_len):
    half_len = transform_len // 2
    sample_idx = jnp.arange(samples, dtype=jnp.int32)[:, None]
    slot_idx = jnp.arange(transform_len, dtype=jnp.int32)[None, :]
    freq_idx = jnp.where(slot_idx < half_len, slot_idx, slot_idx - half_len)
    phases = sample_idx * freq_idx % transform_len
    angles = phases.astype(jnp.float32) * (2.0 * math.pi / transform_len)
    nyquist = jnp.where(sample_idx % 2 == 0, 1.0, -1.0)
    basis = jnp.where(slot_idx < half_len, jnp.cos(angles), jnp.where(slot_idx == half_len, nyquist, -jnp.sin(angles)))
    return basis.astype(jnp.bfloat16)

def inverse_table(transform_len, lag_total):
    half_len = transform_len // 2
    slot_idx = jnp.arange(transform_len, dtype=jnp.int32)[:, None]
    lag_idx = jnp.arange(lag_total, dtype=jnp.int32)[None, :] - lag_total // 2
    freq_idx = jnp.where(slot_idx < half_len, slot_idx, slot_idx - half_len)
    phases = freq_idx * lag_idx % transform_len
    angles = phases.astype(jnp.float32) * (2.0 * math.pi / transform_len)
    weight = jnp.where(freq_idx == 0, 1.0, 2.0) / transform_len
    nyquist = jnp.where(lag_idx % 2 == 0, 1.0, -1.0) / transform_len
    basis = jnp.where(slot_idx < half_len, weight * jnp.cos(angles), jnp.where(slot_idx == half_len, nyquist, -weight * jnp.sin(angles)))
    return basis.astype(jnp.bfloat16)

def spectra_of(normed, basis):
    row_total, comps, samples = normed.shape
    flattened = normed.reshape(row_total * comps, samples)
    spectrum = jnp.dot(flattened, basis, preferred_element_type=jnp.float32)
    return spectrum.astype(jnp.bfloat16).reshape(row_total, comps, basis.shape[1])

def pair_einsum(left_part, right_part):
    return jnp.einsum('icf,jcf->ijf', left_part.astype(jnp.float32), right_part.astype(jnp.float32))

def similarity(left_spec, right_spec, inverse):
    half_len = left_spec.shape[2] // 2
    left_real = left_spec[:, :, :half_len]
    left_imag = left_spec[:, :, half_len:]
    right_real = right_spec[:, :, :half_len]
    right_imag = right_spec[:, :, half_len:]
    above_zero = jnp.arange(half_len, dtype=jnp.int32) >= 1
    right_masked = jnp.where(above_zero, right_imag, jnp.zeros_like(right_imag))
    left_masked = jnp.where(above_zero, left_real, jnp.zeros_like(left_real))
    right_turned = jnp.where(above_zero, -right_real, right_imag)
    even_part = pair_einsum(jnp.concatenate([left_real, left_imag], axis=1), jnp.concatenate([right_real, right_masked], axis=1))
    odd_part = pair_einsum(jnp.concatenate([left_masked, left_imag], axis=1), jnp.concatenate([right_imag, right_turned], axis=1))
    cross_spec = jnp.concatenate([even_part, odd_part], axis=2).astype(jnp.bfloat16)
    left_rows = left_spec.shape[0]
    right_rows = right_spec.shape[0]
    lagged = jnp.dot(cross_spec.reshape(left_rows * right_rows, 2 * half_len), inverse, preferred_element_type=jnp.float32)
    return lax.optimization_barrier(jnp.max(lagged, axis=1)).reshape(left_rows, right_rows)

def reference(templates):
    forward = forward_table(SAMPLES, NFFT)
    inverse = inverse_table(NFFT, LAGS)
    spectrum = spectra_of(normalize(templates), forward)
    block_total = math.gcd(NT, 64)
    pieces = spectrum.reshape(block_total, NT // block_total, COMP, NFFT)
    similar = lax.map(lambda row_piece: similarity(row_piece, spectrum, inverse), pieces)
    return similar.reshape(NT, NT)
```

```python
import functools
import math

import jax
import jax.numpy as jnp
from jax import lax
from jax.experimental import pallas as pl
from jax.experimental.pallas import tpu as pltpu
from jax.sharding import PartitionSpec as P

LAGS = 512
LANES = 128
SUBS = 8
CORES = 2
MESH = pl.DeviceIdType.MESH


def each(count, step):
    if count <= 8:
        for k in range(count):
            step(k)
    else:
        lax.fori_loop(0, count, lambda k, carry: (step(k), carry)[1], 0)


def kernel(
    rows, cols, x_ref, out_ref, stage, gathered, toeplitz, flat, waves, send_sem, recv_sem
):
    n, comps, samples = x_ref.shape
    chunks = samples // LANES
    span = samples + LANES
    width = samples + 2 * LANES
    devices = rows * cols
    tall = rows // CORES
    wide = 2 ** int(math.log2(math.sqrt(cols)))
    deep = cols // wide
    plane = tall * wide
    row = lax.axis_index("row")
    col = lax.axis_index("col")
    my_y, my_core = row // CORES, row % CORES
    my_z, my_x = col // wide, col % wide
    my_xy = my_y * wide + my_x

    def place(xy, z, core):
        return (xy // wide) * CORES + core, z * wide + xy % wide

    def slot_of(xy, z, core):
        r, c = place(xy, z, core)
        return r * cols + c

    def up(k):
        return (my_z + 1 + k) % deep

    def beside(k):
        return (my_xy + 1 + k) % plane

    other = 1 - my_core
    mine = slot_of(my_xy, my_z, my_core)

    barrier = pltpu.get_barrier_semaphore()

    def greet(xy, z, core):
        pl.semaphore_signal(
            barrier, inc=1, device_id=place(xy, z, core), device_id_type=MESH
        )

    each(deep - 1, lambda k: greet(my_xy, up(k), my_core))
    each(plane - 1, lambda k: greet(beside(k), my_z, my_core))
    greet(my_xy, my_z, other)

    normed = []
    for t in range(n):
        x = x_ref[t]
        scale = lax.rsqrt(jnp.mean(x * x, axis=1, keepdims=True) + 1e-06) / math.sqrt(samples)
        rounded = (x * scale).astype(jnp.bfloat16).astype(jnp.float32)
        normed.append(rounded)
        for q in range(chunks):
            stage[pl.ds(t * comps * chunks + q, comps, stride=chunks), :] = rounded[
                :, q * LANES : (q + 1) * LANES
            ]
    gathered[mine] = stage[...].reshape(n * comps, chunks, LANES).astype(jnp.bfloat16)
    pl.semaphore_wait(barrier, deep - 1 + plane - 1 + 1)

    def copy(slot, to, sem):
        return pltpu.make_async_remote_copy(
            src_ref=gathered.at[slot],
            dst_ref=gathered.at[slot],
            send_sem=send_sem.at[sem],
            recv_sem=recv_sem.at[slot],
            device_id=to,
            device_id_type=MESH,
        )

    def to_sibling(slot):
        return copy(slot, place(my_xy, my_z, other), slot)

    def to_plane(slot, z, k):
        return copy(slot, place(beside(k), my_z, my_core), devices + z * plane + k)

    def to_column(k):
        return copy(mine, place(my_xy, up(k), my_core), devices + deep * plane + k)

    def arrived(slot):
        to_sibling(slot).wait_recv()

    each(deep - 1, lambda k: to_column(k).start())
    each(plane - 1, lambda k: to_plane(mine, my_z, k).start())
    to_sibling(mine).start()

    def build(t, c):
        line = jnp.concatenate(
            [normed[t][c : c + 1], jnp.zeros((1, LANES), jnp.float32)], axis=1
        )
        shifted = pltpu.roll(
            jnp.broadcast_to(line, (LANES, span)), 0, axis=1, stride=1, stride_axis=0
        )
        toeplitz[t * LANES : (t + 1) * LANES, c * span : (c + 1) * span] = shifted.astype(
            jnp.bfloat16
        )

    for t in range(1):
        for c in range(comps):
            build(t, c)

    def pass_on(k):
        z = up(k)
        slot = slot_of(my_xy, z, my_core)
        arrived(slot)
        each(plane - 1, lambda m: to_plane(slot, z, m).start())
        to_sibling(slot).start()

    each(deep - 1, pass_on)

    for t in range(1, n):
        for c in range(comps):
            build(t, c)
    rows_block = waves.shape[0]
    for c in range(comps):
        for at in (0, LANES + samples):
            waves[:, c * width + at : c * width + at + LANES] = jnp.zeros(
                (rows_block, LANES), jnp.bfloat16
            )

    def hand_over(k):
        slot = slot_of(beside(k // deep), (my_z + k % deep) % deep, my_core)
        arrived(slot)
        to_sibling(slot).start()

    each_loop = (plane - 1) * deep
    lax.fori_loop(0, each_loop, lambda k, carry: (hand_over(k), carry)[1], 0)

    def from_sibling(k, carry):
        arrived(slot_of(k // deep, k % deep, other))
        return carry

    lax.fori_loop(0, plane * deep, from_sibling, 0)

    def left(k, carry):
        to_sibling(slot_of(k // deep, k % deep, my_core)).wait_send()
        return carry

    lax.fori_loop(0, plane * deep, left, 0)

    def left_plane(k, carry):
        to_plane(mine, k // (plane - 1), k % (plane - 1)).wait_send()
        return carry

    lax.fori_loop(0, deep * (plane - 1), left_plane, 0)
    each(deep - 1, lambda k: to_column(k).wait_send())

    block = rows_block // n
    stride = comps * chunks

    def compare(b):
        flat[...] = (
            gathered[pl.ds(b * block, block)]
            .astype(jnp.float32)
            .reshape(block * n * comps * chunks, LANES)
        )
        for c in range(comps):
            for q in range(chunks):
                at = c * width + (q + 1) * LANES
                waves[:, at : at + LANES] = flat[
                    pl.ds(c * chunks + q, rows_block, stride=stride), :
                ].astype(jnp.bfloat16)

        best = None
        for lag0 in range(-LAGS // 2, LAGS // 2, 2 * LANES):
            low = max(0, -lag0 - LANES)
            total = None
            for c in range(comps):
                left_part = toeplitz[:, c * span + low : c * span + low + samples]
                at = c * width + LANES + low + lag0
                right_part = jnp.concatenate(
                    [waves[:, at : at + samples], waves[:, at + LANES : at + LANES + samples]],
                    axis=0,
                )
                part = lax.dot_general(
                    left_part,
                    right_part,
                    (((1,), (1,)), ((), ())),
                    preferred_element_type=jnp.float32,
                )
                total = part if total is None else total + part
            top = jnp.max(total.reshape(n, LANES, 2 * rows_block), axis=1)
            best = top if best is None else jnp.maximum(best, top)
        out_ref[b] = jnp.maximum(best[:, :rows_block], best[:, rows_block:])

    each(devices // block, compare)


def body(templates):
    n, comps, samples = templates.shape
    rows = lax.axis_size("row")
    cols = lax.axis_size("col")
    devices = rows * cols
    block = math.gcd(devices, 32)
    chunks = samples // LANES
    span = samples + LANES
    width = samples + 2 * LANES
    vmem = pl.BlockSpec(memory_space=pltpu.VMEM)
    out = pl.pallas_call(
        functools.partial(kernel, rows, cols),
        out_shape=jax.ShapeDtypeStruct((devices // block, n, block * n), jnp.float32),
        in_specs=[vmem],
        out_specs=vmem,
        scratch_shapes=[
            pltpu.VMEM((n * comps * chunks, LANES), jnp.float32),
            pltpu.VMEM((devices, n * comps, chunks, LANES), jnp.bfloat16),
            pltpu.VMEM((n * LANES, comps * span), jnp.bfloat16),
            pltpu.VMEM((block * n * comps * chunks, LANES), jnp.float32),
            pltpu.VMEM((block * n, comps * width), jnp.bfloat16),
            pltpu.SemaphoreType.DMA((2 * devices + cols,)),
            pltpu.SemaphoreType.DMA((devices,)),
        ],
        compiler_params=pltpu.CompilerParams(collective_id=0, has_side_effects=True),
    )(templates)
    return out.transpose(1, 0, 2).reshape(n, devices * n)


def solution(mesh):
    placed = (P(("row", "col"), None, None),)
    return jax.shard_map(
        body, mesh=mesh, in_specs=placed, out_specs=P(("row", "col"), None), check_vma=False
    )
```

```python
import functools
import math

import jax
import jax.numpy as jnp
import numpy as np
from jax import lax
from jax.experimental import pallas as pl
from jax.experimental.pallas import tpu as pltpu
from jax.sharding import PartitionSpec as P

LAGS = 512
LANES = 128
SUBS = 8
CORES = 2
MESH = pl.DeviceIdType.MESH


def forward_table(samples, transform_len):
    half_len = transform_len // 2
    sample_idx = np.arange(samples)[:, None]
    slot_idx = np.arange(transform_len)[None, :]
    freq_idx = np.where(slot_idx < half_len, slot_idx, slot_idx - half_len)
    phases = sample_idx * freq_idx % transform_len
    angles = phases.astype(np.float32) * np.float32(2.0 * math.pi / transform_len)
    nyquist = np.where(sample_idx % 2 == 0, 1.0, -1.0)
    basis = np.where(
        slot_idx < half_len,
        np.cos(angles),
        np.where(slot_idx == half_len, nyquist, -np.sin(angles)),
    )
    return basis.astype(np.float32).astype(jnp.bfloat16)


def inverse_table(transform_len, lag_total):
    half_len = transform_len // 2
    slot_idx = np.arange(transform_len)[:, None]
    lag_idx = np.arange(lag_total)[None, :] - lag_total // 2
    freq_idx = np.where(slot_idx < half_len, slot_idx, slot_idx - half_len)
    phases = freq_idx * lag_idx % transform_len
    angles = phases.astype(np.float32) * np.float32(2.0 * math.pi / transform_len)
    weight = (np.where(freq_idx == 0, 1.0, 2.0) / transform_len).astype(np.float32)
    nyquist = np.where(lag_idx % 2 == 0, 1.0, -1.0) / transform_len
    basis = np.where(
        slot_idx < half_len,
        weight * np.cos(angles),
        np.where(slot_idx == half_len, nyquist, -weight * np.sin(angles)),
    )
    return basis.astype(np.float32).astype(jnp.bfloat16)


def each(count, step):
    if count <= 8:
        for k in range(count):
            step(k)
    else:
        lax.fori_loop(0, count, lambda k, carry: (step(k), carry)[1], 0)


def kernel(
    rows,
    cols,
    x_ref,
    forward_hbm,
    inverse_hbm,
    out_ref,
    stage,
    gathered,
    forward,
    inverse,
    flat,
    waves,
    own,
    cross,
    send_sem,
    recv_sem,
    table_sem,
):
    n, comps, samples = x_ref.shape
    chunks = samples // LANES
    half = forward.shape[1] // 2
    tables = [
        pltpu.make_async_copy(forward_hbm, forward, table_sem.at[0]),
        pltpu.make_async_copy(inverse_hbm, inverse, table_sem.at[1]),
    ]
    for table in tables:
        table.start()
    devices = rows * cols
    tall = rows // CORES
    wide = 2 ** int(math.log2(math.sqrt(cols)))
    deep = cols // wide
    plane = tall * wide
    row = lax.axis_index("row")
    col = lax.axis_index("col")
    my_y, my_core = row // CORES, row % CORES
    my_z, my_x = col // wide, col % wide
    my_xy = my_y * wide + my_x

    def place(xy, z, core):
        return (xy // wide) * CORES + core, z * wide + xy % wide

    def slot_of(xy, z, core):
        r, c = place(xy, z, core)
        return r * cols + c

    def up(k):
        return (my_z + 1 + k) % deep

    def beside(k):
        return (my_xy + 1 + k) % plane

    other = 1 - my_core
    mine = slot_of(my_xy, my_z, my_core)

    barrier = pltpu.get_barrier_semaphore()

    def greet(xy, z, core):
        pl.semaphore_signal(
            barrier, inc=1, device_id=place(xy, z, core), device_id_type=MESH
        )

    each(deep - 1, lambda k: greet(my_xy, up(k), my_core))
    each(plane - 1, lambda k: greet(beside(k), my_z, my_core))
    greet(my_xy, my_z, other)

    normed = []
    for t in range(n):
        x = x_ref[t]
        scale = lax.rsqrt(jnp.mean(x * x, axis=1, keepdims=True) + 1e-06) / math.sqrt(samples)
        rounded = (x * scale).astype(jnp.bfloat16).astype(jnp.float32)
        normed.append(rounded)
        for q in range(chunks):
            stage[pl.ds(t * comps * chunks + q, comps, stride=chunks), :] = rounded[
                :, q * LANES : (q + 1) * LANES
            ]
    gathered[mine] = stage[...].reshape(n * comps, chunks, LANES).astype(jnp.bfloat16)
    pl.semaphore_wait(barrier, deep - 1 + plane - 1 + 1)

    def copy(slot, to, sem):
        return pltpu.make_async_remote_copy(
            src_ref=gathered.at[slot],
            dst_ref=gathered.at[slot],
            send_sem=send_sem.at[sem],
            recv_sem=recv_sem.at[slot],
            device_id=to,
            device_id_type=MESH,
        )

    def to_sibling(slot):
        return copy(slot, place(my_xy, my_z, other), slot)

    def to_plane(slot, z, k):
        return copy(slot, place(beside(k), my_z, my_core), devices + z * plane + k)

    def to_column(k):
        return copy(mine, place(my_xy, up(k), my_core), devices + deep * plane + k)

    def arrived(slot):
        to_sibling(slot).wait_recv()

    each(deep - 1, lambda k: to_column(k).start())
    each(plane - 1, lambda k: to_plane(mine, my_z, k).start())
    to_sibling(mine).start()

    def pass_on(k):
        z = up(k)
        slot = slot_of(my_xy, z, my_core)
        arrived(slot)
        each(plane - 1, lambda m: to_plane(slot, z, m).start())
        to_sibling(slot).start()

    each(deep - 1, pass_on)

    tables[0].wait()
    bins = lax.broadcasted_iota(jnp.int32, (1, half), 1)
    local = jnp.concatenate(normed, axis=0)
    pad = -local.shape[0] % 16
    local = jnp.concatenate([local, jnp.zeros((pad, samples), jnp.float32)], axis=0)
    spectrum = jnp.dot(
        local.astype(jnp.bfloat16), forward[...], preferred_element_type=jnp.float32
    )
    spectrum = spectrum.astype(jnp.bfloat16).astype(jnp.float32)
    real, imag = spectrum[:, :half], spectrum[:, half:]
    own[0] = real
    own[1] = jnp.where(bins == 0, 0.0, imag)
    own[2] = jnp.where(bins == 0, imag, real)

    def hand_over(k):
        slot = slot_of(beside(k // deep), (my_z + k % deep) % deep, my_core)
        arrived(slot)
        to_sibling(slot).start()

    each_loop = (plane - 1) * deep
    lax.fori_loop(0, each_loop, lambda k, carry: (hand_over(k), carry)[1], 0)

    def from_sibling(k, carry):
        arrived(slot_of(k // deep, k % deep, other))
        return carry

    lax.fori_loop(0, plane * deep, from_sibling, 0)

    def left(k, carry):
        to_sibling(slot_of(k // deep, k % deep, my_core)).wait_send()
        return carry

    lax.fori_loop(0, plane * deep, left, 0)

    def left_plane(k, carry):
        to_plane(mine, k // (plane - 1), k % (plane - 1)).wait_send()
        return carry

    lax.fori_loop(0, deep * (plane - 1), left_plane, 0)
    each(deep - 1, lambda k: to_column(k).wait_send())

    rows_block = waves.shape[0] // comps
    block = rows_block // n
    stride = comps * chunks
    tables[1].wait()

    def compare(b):
        flat[...] = (
            gathered[pl.ds(b * block, block)]
            .astype(jnp.float32)
            .reshape(block * n * comps * chunks, LANES)
        )
        for c in range(comps):
            for q in range(chunks):
                waves[c * rows_block : (c + 1) * rows_block, q * LANES : (q + 1) * LANES] = flat[
                    pl.ds(c * chunks + q, rows_block, stride=stride), :
                ].astype(jnp.bfloat16)

        for f in range(0, half, LANES):
            g = half + f
            basis = jnp.concatenate(
                [forward[:, f : f + LANES], forward[:, g : g + LANES]], axis=1
            )
            spectra = jnp.dot(waves[...], basis, preferred_element_type=jnp.float32)
            spectra = spectra.astype(jnp.bfloat16).astype(jnp.float32)
            for j in range(0, rows_block, 16):
                for i in range(n):
                    even, odd = 0.0, 0.0
                    for c in range(comps):
                        at = c * rows_block + j
                        real = spectra[at : at + 16, :LANES]
                        imag = spectra[at : at + 16, LANES:]
                        r = i * comps + c
                        plain = own[0, r : r + 1, f : f + LANES]
                        turned = own[1, r : r + 1, f : f + LANES]
                        mixed = own[2, r : r + 1, f : f + LANES]
                        even = even + (plain * real + turned * imag)
                        odd = odd + (mixed * imag - turned * real)
                    at = i * rows_block + j
                    cross[at : at + 16, f : f + LANES] = even.astype(jnp.bfloat16)
                    cross[at : at + 16, g : g + LANES] = odd.astype(jnp.bfloat16)

        lagged = jnp.dot(cross[...], inverse[...], preferred_element_type=jnp.float32)
        top = lagged[:, :LANES]
        for at in range(LANES, LAGS, LANES):
            top = jnp.maximum(top, lagged[:, at : at + LANES])
        for i in range(n):
            part = top[i * rows_block : (i + 1) * rows_block]
            out_ref[b, i : i + 1] = jnp.max(part.T, axis=0, keepdims=True)

    each(devices // block, compare)


def body(templates):
    n, comps, samples = templates.shape
    rows = lax.axis_size("row")
    cols = lax.axis_size("col")
    devices = rows * cols
    block = math.gcd(devices, 32)
    chunks = samples // LANES
    transform_len = samples + LAGS // 2
    forward = forward_table(samples, transform_len)
    inverse = inverse_table(transform_len, LAGS)
    vmem = pl.BlockSpec(memory_space=pltpu.VMEM)
    out = pl.pallas_call(
        functools.partial(kernel, rows, cols),
        out_shape=jax.ShapeDtypeStruct((devices // block, n, block * n), jnp.float32),
        in_specs=[vmem, pl.BlockSpec(memory_space=pl.ANY), pl.BlockSpec(memory_space=pl.ANY)],
        out_specs=vmem,
        scratch_shapes=[
            pltpu.VMEM((n * comps * chunks, LANES), jnp.float32),
            pltpu.VMEM((devices, n * comps, chunks, LANES), jnp.bfloat16),
            pltpu.VMEM(forward.shape, jnp.bfloat16),
            pltpu.VMEM(inverse.shape, jnp.bfloat16),
            pltpu.VMEM((block * n * comps * chunks, LANES), jnp.float32),
            pltpu.VMEM((comps * block * n, samples), jnp.bfloat16),
            pltpu.VMEM((3, n * comps + -(n * comps) % 16, transform_len // 2), jnp.float32),
            pltpu.VMEM((n * block * n, transform_len), jnp.bfloat16),
            pltpu.SemaphoreType.DMA((2 * devices + cols,)),
            pltpu.SemaphoreType.DMA((devices,)),
            pltpu.SemaphoreType.DMA((2,)),
        ],
        compiler_params=pltpu.CompilerParams(collective_id=0, has_side_effects=True),
    )(templates, forward, inverse)
    return out.transpose(1, 0, 2).reshape(n, devices * n)


def solution(mesh):
    placed = (P(("row", "col"), None, None),)
    return jax.shard_map(
        body, mesh=mesh, in_specs=placed, out_specs=P(("row", "col"), None), check_vma=False
    )
```

```python
import functools
import math

import jax
import jax.numpy as jnp
import numpy as np
from jax import lax
from jax.experimental import pallas as pl
from jax.experimental.pallas import tpu as pltpu
from jax.sharding import PartitionSpec as P

LAGS = 512
LANES = 128
SUBS = 8
CORES = 2
MESH = pl.DeviceIdType.MESH


def forward_table(samples, transform_len):
    half_len = transform_len // 2
    sample_idx = np.arange(samples)[:, None]
    slot_idx = np.arange(transform_len)[None, :]
    freq_idx = np.where(slot_idx < half_len, slot_idx, slot_idx - half_len)
    phases = sample_idx * freq_idx % transform_len
    angles = phases.astype(np.float32) * np.float32(2.0 * math.pi / transform_len)
    nyquist = np.where(sample_idx % 2 == 0, 1.0, -1.0)
    basis = np.where(
        slot_idx < half_len,
        np.cos(angles),
        np.where(slot_idx == half_len, nyquist, -np.sin(angles)),
    )
    return basis.astype(np.float32).astype(jnp.bfloat16)


def inverse_table(transform_len, lag_total):
    half_len = transform_len // 2
    slot_idx = np.arange(transform_len)[:, None]
    lag_idx = np.arange(lag_total)[None, :] - lag_total // 2
    freq_idx = np.where(slot_idx < half_len, slot_idx, slot_idx - half_len)
    phases = freq_idx * lag_idx % transform_len
    angles = phases.astype(np.float32) * np.float32(2.0 * math.pi / transform_len)
    weight = (np.where(freq_idx == 0, 1.0, 2.0) / transform_len).astype(np.float32)
    nyquist = np.where(lag_idx % 2 == 0, 1.0, -1.0) / transform_len
    basis = np.where(
        slot_idx < half_len,
        weight * np.cos(angles),
        np.where(slot_idx == half_len, nyquist, -weight * np.sin(angles)),
    )
    return basis.astype(np.float32).astype(jnp.bfloat16)


def each(count, step):
    if count <= 8:
        for k in range(count):
            step(k)
    else:
        lax.fori_loop(0, count, lambda k, carry: (step(k), carry)[1], 0)


def kernel(
    rows,
    cols,
    x_ref,
    forward_hbm,
    inverse_hbm,
    out_ref,
    stage,
    gathered,
    forward,
    inverse,
    flat,
    waves,
    own,
    cross,
    outgoing,
    incoming,
    send_sem,
    recv_sem,
    table_sem,
    result_sem,
):
    n, comps, samples = x_ref.shape
    chunks = samples // LANES
    lines = n * comps * chunks
    half = forward.shape[1] // 2
    tables = [
        pltpu.make_async_copy(forward_hbm, forward, table_sem.at[0]),
        pltpu.make_async_copy(inverse_hbm, inverse, table_sem.at[1]),
    ]
    for table in tables:
        table.start()
    tall = rows // CORES
    wide = 2 ** int(math.log2(math.sqrt(cols)))
    deep = cols // wide
    plane = tall * wide
    slots = plane * deep
    row = lax.axis_index("row")
    col = lax.axis_index("col")
    my_y, my_core = row // CORES, row % CORES
    my_z, my_x = col // wide, col % wide
    my_xy = my_y * wide + my_x

    def place(xy, z, core):
        return (xy // wide) * CORES + core, z * wide + xy % wide

    def slot_of(xy, z):
        return (xy // wide) * cols + z * wide + xy % wide

    def up(k):
        if deep & (deep - 1):
            return (my_z + 1 + k) % deep
        z, bit = 0, 1
        while bit < deep:
            z, bit = z + (my_z // bit + (1 + k) // bit) % 2 * bit, bit * 2
        return z

    def beside(k):
        return (my_xy + 1 + k) % plane

    other = 1 - my_core
    mine = slot_of(my_xy, my_z)

    barrier = pltpu.get_barrier_semaphore()

    def greet(xy, z, core):
        pl.semaphore_signal(
            barrier, inc=1, device_id=place(xy, z, core), device_id_type=MESH
        )

    each(deep - 1, lambda k: greet(my_xy, up(k), my_core))
    each(plane - 1, lambda k: greet(beside(k), my_z, my_core))
    greet(my_xy, my_z, other)

    for t in range(n):
        x = x_ref[t]
        scale = lax.rsqrt(jnp.mean(x * x, axis=1, keepdims=True) + 1e-06) / math.sqrt(samples)
        rounded = (x * scale).astype(jnp.bfloat16).astype(jnp.float32)
        for q in range(chunks):
            stage[pl.ds(t * comps * chunks + q, comps, stride=chunks), :] = rounded[
                :, q * LANES : (q + 1) * LANES
            ]
    gathered[mine] = stage[:lines].reshape(n * comps, chunks, LANES).astype(jnp.bfloat16)
    pl.semaphore_wait(barrier, deep - 1 + plane - 1 + 1)

    def copy(slot, to, sem, landing=None):
        landing = slot if landing is None else landing
        return pltpu.make_async_remote_copy(
            src_ref=gathered.at[slot],
            dst_ref=gathered.at[landing],
            send_sem=send_sem.at[sem],
            recv_sem=recv_sem.at[landing],
            device_id=to,
            device_id_type=MESH,
        )

    def to_plane(slot, z, k):
        return copy(slot, place(beside(k), my_z, my_core), z * plane + k)

    def to_column(k):
        return copy(mine, place(my_xy, up(k), my_core), slots + k)

    def to_sibling():
        return copy(mine, place(my_xy, my_z, other), slots + deep, slots)

    def arrived(slot):
        copy(slot, place(my_xy, my_z, other), slots + deep).wait_recv()

    each(deep - 1, lambda k: to_column(deep - 2 - k).start())
    to_sibling().start()
    each(plane - 1, lambda k: to_plane(mine, my_z, k).start())

    arrived(slots)
    stage[lines:] = gathered[slots].astype(jnp.float32).reshape(lines, LANES)
    tables[0].wait()
    local = jnp.concatenate(
        [stage[pl.ds(q, CORES * n * comps, stride=chunks), :] for q in range(chunks)], axis=1
    )
    pad = own.shape[1] - local.shape[0]
    local = jnp.concatenate([local, jnp.zeros((pad, samples), jnp.float32)], axis=0)
    spectrum = jnp.dot(
        local.astype(jnp.bfloat16), forward[...], preferred_element_type=jnp.float32
    )
    spectrum = spectrum.astype(jnp.bfloat16).astype(jnp.float32)
    real, imag = spectrum[:, :half], spectrum[:, half:]
    bins = lax.broadcasted_iota(jnp.int32, (1, half), 1)
    own[0] = real
    own[1] = jnp.where(bins == 0, 0.0, imag)
    own[2] = jnp.where(bins == 0, imag, real)

    def pass_on(k):
        z = up(k)
        slot = slot_of(my_xy, z)
        arrived(slot)
        each(plane - 1, lambda m: to_plane(slot, z, m).start())

    each(deep - 1, pass_on)
    tables[1].wait()
    each(
        (plane - 1) * deep,
        lambda k: arrived(slot_of(beside(k // deep), (my_z + k % deep) % deep)),
    )

    rows_block = waves.shape[0] // comps
    block = rows_block // n
    blocks = slots // block
    stride = comps * chunks

    def result(b):
        return pltpu.make_async_remote_copy(
            src_ref=outgoing.at[b],
            dst_ref=incoming.at[b],
            send_sem=result_sem.at[b],
            recv_sem=result_sem.at[blocks + b],
            device_id=place(my_xy, my_z, other),
            device_id_type=MESH,
        )

    def compare(b):
        flat[...] = (
            gathered[pl.ds(b * block, block)]
            .astype(jnp.float32)
            .reshape(block * n * comps * chunks, LANES)
        )
        for c in range(comps):
            for q in range(chunks):
                waves[c * rows_block : (c + 1) * rows_block, q * LANES : (q + 1) * LANES] = flat[
                    pl.ds(c * chunks + q, rows_block, stride=stride), :
                ].astype(jnp.bfloat16)

        for f in range(0, half, LANES):
            g = half + f
            basis = jnp.concatenate(
                [forward[:, f : f + LANES], forward[:, g : g + LANES]], axis=1
            )
            spectra = jnp.dot(waves[...], basis, preferred_element_type=jnp.float32)
            spectra = spectra.astype(jnp.bfloat16).astype(jnp.float32)
            for j in range(0, rows_block, 16):
                for i in range(CORES * n):
                    even, odd = 0.0, 0.0
                    for c in range(comps):
                        at = c * rows_block + j
                        real = spectra[at : at + 16, :LANES]
                        imag = spectra[at : at + 16, LANES:]
                        r = i * comps + c
                        plain = own[0, r : r + 1, f : f + LANES]
                        turned = own[1, r : r + 1, f : f + LANES]
                        mixed = own[2, r : r + 1, f : f + LANES]
                        even = even + (plain * real + turned * imag)
                        odd = odd + (mixed * imag - turned * real)
                    at = i * rows_block + j
                    cross[at : at + 16, f : f + LANES] = even.astype(jnp.bfloat16)
                    cross[at : at + 16, g : g + LANES] = odd.astype(jnp.bfloat16)

        def similar(core):
            first = core * n * rows_block
            lagged = jnp.dot(
                cross[first : first + n * rows_block],
                inverse[...],
                preferred_element_type=jnp.float32,
            )
            top = lagged[:, :LANES]
            for at in range(LANES, LAGS, LANES):
                top = jnp.maximum(top, lagged[:, at : at + LANES])
            flipped = jnp.max(top.T, axis=0, keepdims=True)
            return jnp.concatenate(
                [flipped[:, i * rows_block : (i + 1) * rows_block] for i in range(n)], axis=0
            )

        outgoing[b] = similar(1)
        result(b).start()
        out = similar(0)
        result(b).wait_recv()
        theirs = incoming[b]
        low = jnp.where(my_core == 0, out, theirs)
        high = jnp.where(my_core == 0, theirs, out)
        if blocks == 1:
            part = cols * n
            out_ref[...] = jnp.concatenate(
                [
                    kind[:, y * part : (y + 1) * part]
                    for y in range(tall)
                    for kind in (low, high)
                ],
                axis=1,
            )
        else:
            out_ref[b, 0] = low
            out_ref[b, 1] = high
        result(b).wait_send()

    each(blocks, compare)

    each(
        deep * (plane - 1),
        lambda k: to_plane(mine, k // (plane - 1), k % (plane - 1)).wait_send(),
    )
    each(deep - 1, lambda k: to_column(k).wait_send())
    to_sibling().wait_send()


def body(templates):
    n, comps, samples = templates.shape
    rows = lax.axis_size("row")
    cols = lax.axis_size("col")
    slots = rows * cols // CORES
    block = math.gcd(slots, 16)
    blocks = slots // block
    chunks = samples // LANES
    transform_len = samples + LAGS // 2
    forward = forward_table(samples, transform_len)
    inverse = inverse_table(transform_len, LAGS)
    vmem = pl.BlockSpec(memory_space=pltpu.VMEM)
    hbm = pl.BlockSpec(memory_space=pl.ANY)
    local = CORES * n * comps
    shape = (n, CORES * slots * n) if blocks == 1 else (blocks, CORES, n, block * n)
    out = pl.pallas_call(
        functools.partial(kernel, rows, cols),
        out_shape=jax.ShapeDtypeStruct(shape, jnp.float32),
        in_specs=[vmem, hbm, hbm],
        out_specs=vmem,
        scratch_shapes=[
            pltpu.VMEM((CORES * n * comps * chunks, LANES), jnp.float32),
            pltpu.VMEM((slots + 1, n * comps, chunks, LANES), jnp.bfloat16),
            pltpu.VMEM(forward.shape, jnp.bfloat16),
            pltpu.VMEM(inverse.shape, jnp.bfloat16),
            pltpu.VMEM((block * n * comps * chunks, LANES), jnp.float32),
            pltpu.VMEM((comps * block * n, samples), jnp.bfloat16),
            pltpu.VMEM((3, local + -local % 16, transform_len // 2), jnp.float32),
            pltpu.VMEM((CORES * n * block * n, transform_len), jnp.bfloat16),
            pltpu.VMEM((blocks, n, block * n), jnp.float32),
            pltpu.VMEM((blocks, n, block * n), jnp.float32),
            pltpu.SemaphoreType.DMA((slots + cols + 1,)),
            pltpu.SemaphoreType.DMA((slots + 1,)),
            pltpu.SemaphoreType.DMA((2,)),
            pltpu.SemaphoreType.DMA((2 * blocks,)),
        ],
        compiler_params=pltpu.CompilerParams(collective_id=0, has_side_effects=True),
    )(templates, forward, inverse)
    if blocks == 1:
        return out
    out = out.transpose(2, 1, 0, 3).reshape(n, CORES, rows // CORES, cols * n)
    return out.transpose(0, 2, 1, 3).reshape(n, CORES * slots * n)


def solution(mesh):
    placed = (P(("row", "col"), None, None),)
    return jax.shard_map(
        body, mesh=mesh, in_specs=placed, out_specs=P(("row", "col"), None), check_vma=False
    )
```

```python
import functools
import math

import jax
import jax.numpy as jnp
import numpy as np
from jax import lax
from jax.experimental import pallas as pl
from jax.experimental.pallas import tpu as pltpu
from jax.sharding import PartitionSpec as P

LAGS = 512
LANES = 128
SUBS = 8
CORES = 2
MESH = pl.DeviceIdType.MESH


def forward_table(samples, transform_len):
    half_len = transform_len // 2
    sample_idx = np.arange(samples)[:, None]
    slot_idx = np.arange(transform_len)[None, :]
    freq_idx = np.where(slot_idx < half_len, slot_idx, slot_idx - half_len)
    phases = sample_idx * freq_idx % transform_len
    angles = phases.astype(np.float32) * np.float32(2.0 * math.pi / transform_len)
    nyquist = np.where(sample_idx % 2 == 0, 1.0, -1.0)
    basis = np.where(
        slot_idx < half_len,
        np.cos(angles),
        np.where(slot_idx == half_len, nyquist, -np.sin(angles)),
    )
    return basis.astype(np.float32).astype(jnp.bfloat16)


def inverse_table(transform_len, lag_total):
    half_len = transform_len // 2
    slot_idx = np.arange(transform_len)[:, None]
    lag_idx = np.arange(lag_total)[None, :] - lag_total // 2
    freq_idx = np.where(slot_idx < half_len, slot_idx, slot_idx - half_len)
    phases = freq_idx * lag_idx % transform_len
    angles = phases.astype(np.float32) * np.float32(2.0 * math.pi / transform_len)
    weight = (np.where(freq_idx == 0, 1.0, 2.0) / transform_len).astype(np.float32)
    nyquist = np.where(lag_idx % 2 == 0, 1.0, -1.0) / transform_len
    basis = np.where(
        slot_idx < half_len,
        weight * np.cos(angles),
        np.where(slot_idx == half_len, nyquist, -weight * np.sin(angles)),
    )
    return basis.astype(np.float32).astype(jnp.bfloat16)


def each(count, step):
    if count <= 8:
        for k in range(count):
            step(k)
    else:
        lax.fori_loop(0, count, lambda k, carry: (step(k), carry)[1], 0)


def kernel(
    rows,
    cols,
    x_hbm,
    forward_hbm,
    inverse_hbm,
    out_ref,
    x_ref,
    stage,
    gathered,
    forward,
    inverse,
    flat,
    waves,
    own,
    spectra,
    cross,
    outgoing,
    incoming,
    send_sem,
    recv_sem,
    table_sem,
    result_sem,
):
    n, comps, samples = x_ref.shape
    chunks = samples // LANES
    lines = n * comps * chunks
    half = forward.shape[1] // 2
    tables = [
        pltpu.make_async_copy(forward_hbm, forward, table_sem.at[0]),
        pltpu.make_async_copy(inverse_hbm, inverse, table_sem.at[1]),
    ]
    tall = rows // CORES
    wide = 2 ** int(math.log2(math.sqrt(cols)))
    deep = cols // wide
    plane = tall * wide
    slots = plane * deep
    row = lax.axis_index("row")
    col = lax.axis_index("col")
    my_y, my_core = row // CORES, row % CORES
    my_z, my_x = col // wide, col % wide
    my_xy = my_y * wide + my_x

    def place(xy, z, core):
        return (xy // wide) * CORES + core, z * wide + xy % wide

    def slot_of(xy, z):
        return (xy // wide) * cols + z * wide + xy % wide

    def up(k):
        if deep & (deep - 1):
            return (my_z + 1 + k) % deep
        z, bit = 0, 1
        while bit < deep:
            z, bit = z + (my_z // bit + (1 + k) // bit) % 2 * bit, bit * 2
        return z

    def beside(k):
        return (my_xy + 1 + k) % plane

    other = 1 - my_core
    mine = slot_of(my_xy, my_z)

    barrier = pltpu.get_barrier_semaphore()

    def greet(xy, z, core):
        pl.semaphore_signal(
            barrier, inc=1, device_id=place(xy, z, core), device_id_type=MESH
        )

    each(deep - 1, lambda k: greet(my_xy, up(k), my_core))
    each(plane - 1, lambda k: greet(beside(k), my_z, my_core))
    greet(my_xy, my_z, other)

    taken = pltpu.make_async_copy(x_hbm, x_ref, table_sem.at[2])
    taken.start()
    for table in tables:
        table.start()
    taken.wait()

    for t in range(n):
        x = x_ref[t]
        scale = lax.rsqrt(jnp.mean(x * x, axis=1, keepdims=True) + 1e-06) / math.sqrt(samples)
        rounded = (x * scale).astype(jnp.bfloat16).astype(jnp.float32)
        for q in range(chunks):
            stage[pl.ds(t * comps * chunks + q, comps, stride=chunks), :] = rounded[
                :, q * LANES : (q + 1) * LANES
            ]
    gathered[mine] = stage[:lines].reshape(n * comps, chunks, LANES).astype(jnp.bfloat16)
    pl.semaphore_wait(barrier, deep - 1 + plane - 1 + 1)

    def copy(slot, to, sem, landing=None):
        landing = slot if landing is None else landing
        return pltpu.make_async_remote_copy(
            src_ref=gathered.at[slot],
            dst_ref=gathered.at[landing],
            send_sem=send_sem.at[sem],
            recv_sem=recv_sem.at[landing],
            device_id=to,
            device_id_type=MESH,
        )

    def to_plane(slot, z, k):
        return copy(slot, place(beside(k), my_z, my_core), z * plane + k)

    def to_column(k):
        return copy(mine, place(my_xy, up(k), my_core), slots + k)

    def to_sibling():
        return copy(mine, place(my_xy, my_z, other), slots + deep, slots)

    def arrived(slot):
        copy(slot, place(my_xy, my_z, other), slots + deep).wait_recv()

    each(deep - 1, lambda k: to_column(deep - 2 - k).start())
    to_sibling().start()
    each(plane - 1, lambda k: to_plane(mine, my_z, k).start())

    arrived(slots)
    stage[lines:] = gathered[slots].astype(jnp.float32).reshape(lines, LANES)
    tables[0].wait()
    local = jnp.concatenate(
        [stage[pl.ds(q, CORES * n * comps, stride=chunks), :] for q in range(chunks)], axis=1
    )
    pad = own.shape[1] - local.shape[0]
    local = jnp.concatenate([local, jnp.zeros((pad, samples), jnp.float32)], axis=0)
    spectrum = jnp.dot(
        local.astype(jnp.bfloat16), forward[...], preferred_element_type=jnp.float32
    )
    spectrum = spectrum.astype(jnp.bfloat16).astype(jnp.float32)
    real, imag = spectrum[:, :half], spectrum[:, half:]
    bins = lax.broadcasted_iota(jnp.int32, (1, half), 1)
    own[0] = real
    own[1] = jnp.where(bins == 0, 0.0, imag)
    own[2] = jnp.where(bins == 0, imag, real)

    def pass_on(k):
        z = up(k)
        slot = slot_of(my_xy, z)
        arrived(slot)
        each(plane - 1, lambda m: to_plane(slot, z, m).start())

    each(deep - 1, pass_on)
    tables[1].wait()
    each(
        (plane - 1) * deep,
        lambda k: arrived(slot_of(beside(k // deep), (my_z + k % deep) % deep)),
    )

    rows_block = waves.shape[0] // comps
    block = rows_block // n
    blocks = slots // block
    stride = comps * chunks

    def result(b):
        return pltpu.make_async_remote_copy(
            src_ref=outgoing.at[b],
            dst_ref=incoming.at[b],
            send_sem=result_sem.at[b],
            recv_sem=result_sem.at[blocks + b],
            device_id=place(my_xy, my_z, other),
            device_id_type=MESH,
        )

    def compare(b):
        flat[...] = (
            gathered[pl.ds(b * block, block)]
            .astype(jnp.float32)
            .reshape(block * n * comps * chunks, LANES)
        )
        for c in range(comps):
            for q in range(chunks):
                waves[c * rows_block : (c + 1) * rows_block, q * LANES : (q + 1) * LANES] = flat[
                    pl.ds(c * chunks + q, rows_block, stride=stride), :
                ].astype(jnp.bfloat16)

        for f in range(0, half, LANES):
            g = half + f
            basis = jnp.concatenate(
                [forward[:, f : f + LANES], forward[:, g : g + LANES]], axis=1
            )
            found = jnp.dot(waves[...], basis, preferred_element_type=jnp.float32)
            found = found.astype(jnp.bfloat16).astype(jnp.float32)
            spectra[:, f : f + LANES] = found[:, :LANES]
            spectra[:, g : g + LANES] = found[:, LANES:]

        def multiply(core):
            for f in range(0, half, LANES):
                g = half + f
                for j in range(0, rows_block, 16):
                    for i in range(core * n, (core + 1) * n):
                        even, odd = 0.0, 0.0
                        for c in range(comps):
                            at = c * rows_block + j
                            real = spectra[at : at + 16, f : f + LANES]
                            imag = spectra[at : at + 16, g : g + LANES]
                            r = i * comps + c
                            plain = own[0, r : r + 1, f : f + LANES]
                            turned = own[1, r : r + 1, f : f + LANES]
                            mixed = own[2, r : r + 1, f : f + LANES]
                            even = even + (plain * real + turned * imag)
                            odd = odd + (mixed * imag - turned * real)
                        at = i * rows_block + j
                        cross[at : at + 16, f : f + LANES] = even.astype(jnp.bfloat16)
                        cross[at : at + 16, g : g + LANES] = odd.astype(jnp.bfloat16)

        def similar(core):
            multiply(core)
            first = core * n * rows_block
            lagged = jnp.dot(
                cross[first : first + n * rows_block],
                inverse[...],
                preferred_element_type=jnp.float32,
            )
            top = lagged[:, :LANES]
            for at in range(LANES, LAGS, LANES):
                top = jnp.maximum(top, lagged[:, at : at + LANES])
            flipped = jnp.max(top.T, axis=0, keepdims=True)
            return jnp.concatenate(
                [flipped[:, i * rows_block : (i + 1) * rows_block] for i in range(n)], axis=0
            )

        outgoing[b] = similar(1)
        result(b).start()
        out = similar(0)
        result(b).wait_recv()
        theirs = incoming[b]
        low = jnp.where(my_core == 0, out, theirs)
        high = jnp.where(my_core == 0, theirs, out)
        if blocks == 1:
            part = cols * n
            out_ref[...] = jnp.concatenate(
                [
                    kind[:, y * part : (y + 1) * part]
                    for y in range(tall)
                    for kind in (low, high)
                ],
                axis=1,
            )
        else:
            out_ref[b, 0] = low
            out_ref[b, 1] = high
        result(b).wait_send()

    each(blocks, compare)

    each(
        deep * (plane - 1),
        lambda k: to_plane(mine, k // (plane - 1), k % (plane - 1)).wait_send(),
    )
    each(deep - 1, lambda k: to_column(k).wait_send())
    to_sibling().wait_send()


def body(templates):
    n, comps, samples = templates.shape
    rows = lax.axis_size("row")
    cols = lax.axis_size("col")
    slots = rows * cols // CORES
    block = math.gcd(slots, 16)
    blocks = slots // block
    chunks = samples // LANES
    transform_len = samples + LAGS // 2
    forward = forward_table(samples, transform_len)
    inverse = inverse_table(transform_len, LAGS)
    vmem = pl.BlockSpec(memory_space=pltpu.VMEM)
    hbm = pl.BlockSpec(memory_space=pltpu.HBM)
    local = CORES * n * comps
    shape = (n, CORES * slots * n) if blocks == 1 else (blocks, CORES, n, block * n)
    out = pl.pallas_call(
        functools.partial(kernel, rows, cols),
        out_shape=pltpu.VMEM(shape, jnp.float32),
        in_specs=[hbm, hbm, hbm],
        out_specs=vmem,
        scratch_shapes=[
            pltpu.VMEM(templates.shape, jnp.float32),
            pltpu.VMEM((CORES * n * comps * chunks, LANES), jnp.float32),
            pltpu.VMEM((slots + 1, n * comps, chunks, LANES), jnp.bfloat16),
            pltpu.VMEM(forward.shape, jnp.bfloat16),
            pltpu.VMEM(inverse.shape, jnp.bfloat16),
            pltpu.VMEM((block * n * comps * chunks, LANES), jnp.float32),
            pltpu.VMEM((comps * block * n, samples), jnp.bfloat16),
            pltpu.VMEM((3, local + -local % 16, transform_len // 2), jnp.float32),
            pltpu.VMEM((comps * block * n, transform_len), jnp.float32),
            pltpu.VMEM((CORES * n * block * n, transform_len), jnp.bfloat16),
            pltpu.VMEM((blocks, n, block * n), jnp.float32),
            pltpu.VMEM((blocks, n, block * n), jnp.float32),
            pltpu.SemaphoreType.DMA((slots + cols + 1,)),
            pltpu.SemaphoreType.DMA((slots + 1,)),
            pltpu.SemaphoreType.DMA((3,)),
            pltpu.SemaphoreType.DMA((2 * blocks,)),
        ],
        compiler_params=pltpu.CompilerParams(collective_id=0, has_side_effects=True),
    )(templates, forward, inverse)
    if blocks == 1:
        return out
    out = out.transpose(2, 1, 0, 3).reshape(n, CORES, rows // CORES, cols * n)
    return out.transpose(0, 2, 1, 3).reshape(n, CORES * slots * n)


def solution(mesh):
    placed = (P(("row", "col"), None, None),)
    return jax.shard_map(
        body, mesh=mesh, in_specs=placed, out_specs=P(("row", "col"), None), check_vma=False
    )
```

```python
import functools
import math

import jax
import jax.numpy as jnp
import numpy as np
from jax import lax
from jax.experimental import pallas as pl
from jax.experimental.pallas import tpu as pltpu
from jax.sharding import PartitionSpec as P

LAGS = 512
LANES = 128
SUBS = 8
CORES = 2
MESH = pl.DeviceIdType.MESH


def forward_table(samples, transform_len):
    half_len = transform_len // 2
    sample_idx = np.arange(samples)[:, None]
    slot_idx = np.arange(transform_len)[None, :]
    freq_idx = np.where(slot_idx < half_len, slot_idx, slot_idx - half_len)
    phases = sample_idx * freq_idx % transform_len
    angles = phases.astype(np.float32) * np.float32(2.0 * math.pi / transform_len)
    nyquist = np.where(sample_idx % 2 == 0, 1.0, -1.0)
    basis = np.where(
        slot_idx < half_len,
        np.cos(angles),
        np.where(slot_idx == half_len, nyquist, -np.sin(angles)),
    )
    return basis.astype(np.float32).astype(jnp.bfloat16)


def inverse_table(transform_len, lag_total):
    half_len = transform_len // 2
    slot_idx = np.arange(transform_len)[:, None]
    lag_idx = np.arange(lag_total)[None, :] - lag_total // 2
    freq_idx = np.where(slot_idx < half_len, slot_idx, slot_idx - half_len)
    phases = freq_idx * lag_idx % transform_len
    angles = phases.astype(np.float32) * np.float32(2.0 * math.pi / transform_len)
    weight = (np.where(freq_idx == 0, 1.0, 2.0) / transform_len).astype(np.float32)
    nyquist = np.where(lag_idx % 2 == 0, 1.0, -1.0) / transform_len
    basis = np.where(
        slot_idx < half_len,
        weight * np.cos(angles),
        np.where(slot_idx == half_len, nyquist, -weight * np.sin(angles)),
    )
    return basis.astype(np.float32).astype(jnp.bfloat16)


def each(count, step):
    if count <= 8:
        for k in range(count):
            step(k)
    else:
        lax.fori_loop(0, count, lambda k, carry: (step(k), carry)[1], 0)


def kernel(
    rows,
    cols,
    x_hbm,
    forward_hbm,
    inverse_hbm,
    out_ref,
    x_ref,
    stage,
    gathered,
    forward,
    inverse,
    flat,
    waves,
    own,
    spectra,
    cross,
    outgoing,
    incoming,
    send_sem,
    recv_sem,
    table_sem,
    result_sem,
):
    n, comps, samples = x_ref.shape
    chunks = samples // LANES
    lines = n * comps * chunks
    half = forward.shape[1] // 2
    tables = [
        pltpu.make_async_copy(forward_hbm, forward, table_sem.at[0]),
        pltpu.make_async_copy(inverse_hbm, inverse, table_sem.at[1]),
    ]
    tall = rows // CORES
    wide = 2 ** int(math.log2(math.sqrt(cols)))
    deep = cols // wide
    plane = tall * wide
    slots = plane * deep
    row = lax.axis_index("row")
    col = lax.axis_index("col")
    my_y, my_core = row // CORES, row % CORES
    my_z, my_x = col // wide, col % wide
    my_xy = my_y * wide + my_x

    def place(xy, z, core):
        return (xy // wide) * CORES + core, z * wide + xy % wide

    def slot_of(xy, z):
        return (xy // wide) * cols + z * wide + xy % wide

    def partner(me, count, k):
        if count & (count - 1):
            return (me + k) % count
        found, bit = 0, 1
        while bit < count:
            found, bit = found + (me // bit + k // bit) % 2 * bit, bit * 2
        return found

    def up(k):
        return partner(my_z, deep, 1 + k)

    def beside(k):
        return partner(my_xy, plane, plane - 1 - k)

    other = 1 - my_core
    mine = slot_of(my_xy, my_z)

    barrier = pltpu.get_barrier_semaphore()

    def greet(xy, z, core):
        pl.semaphore_signal(
            barrier, inc=1, device_id=place(xy, z, core), device_id_type=MESH
        )

    each(deep - 1, lambda k: greet(my_xy, up(k), my_core))
    each(plane - 1, lambda k: greet(beside(k), my_z, my_core))
    greet(my_xy, my_z, other)

    taken = pltpu.make_async_copy(x_hbm, x_ref, table_sem.at[2])
    taken.start()
    for table in tables:
        table.start()
    taken.wait()

    for t in range(n):
        x = x_ref[t]
        scale = lax.rsqrt(jnp.mean(x * x, axis=1, keepdims=True) + 1e-06) / math.sqrt(samples)
        rounded = (x * scale).astype(jnp.bfloat16).astype(jnp.float32)
        for q in range(chunks):
            stage[pl.ds(t * comps * chunks + q, comps, stride=chunks), :] = rounded[
                :, q * LANES : (q + 1) * LANES
            ]
    gathered[mine] = stage[:lines].reshape(n * comps, chunks, LANES).astype(jnp.bfloat16)
    pl.semaphore_wait(barrier, deep - 1 + plane - 1 + 1)

    def copy(slot, to, sem, landing=None):
        landing = slot if landing is None else landing
        return pltpu.make_async_remote_copy(
            src_ref=gathered.at[slot],
            dst_ref=gathered.at[landing],
            send_sem=send_sem.at[sem],
            recv_sem=recv_sem.at[landing],
            device_id=to,
            device_id_type=MESH,
        )

    def to_plane(slot, z, k):
        return copy(slot, place(beside(k), my_z, my_core), z * plane + k)

    def to_column(k):
        return copy(mine, place(my_xy, up(k), my_core), slots + k)

    def to_sibling():
        return copy(mine, place(my_xy, my_z, other), slots + deep, slots)

    def arrived(slot):
        copy(slot, place(my_xy, my_z, other), slots + deep).wait_recv()

    each(deep - 1, lambda k: to_column(deep - 2 - k).start())
    to_sibling().start()
    each(plane - 1, lambda k: to_plane(mine, my_z, k).start())

    rows_block = waves.shape[0] // comps
    block = rows_block // n
    blocks = slots // block

    def unpack(slot):
        at = pl.multiple_of(slot * lines, SUBS)
        flat[pl.ds(at, lines), :] = gathered[slot].astype(jnp.float32).reshape(lines, LANES)

    def pass_on(k):
        z = up(k)
        slot = slot_of(my_xy, z)
        arrived(slot)
        each(plane - 1, lambda m: to_plane(slot, z, m).start())

    each(deep - 1, pass_on)
    arrived(slots)
    stage[lines:] = gathered[slots].astype(jnp.float32).reshape(lines, LANES)
    tables[0].wait()
    local = jnp.concatenate(
        [stage[pl.ds(q, CORES * n * comps, stride=chunks), :] for q in range(chunks)], axis=1
    )
    pad = own.shape[1] - local.shape[0]
    local = jnp.concatenate([local, jnp.zeros((pad, samples), jnp.float32)], axis=0)
    spectrum = jnp.dot(
        local.astype(jnp.bfloat16), forward[...], preferred_element_type=jnp.float32
    )
    spectrum = spectrum.astype(jnp.bfloat16).astype(jnp.float32)
    real, imag = spectrum[:, :half], spectrum[:, half:]
    bins = lax.broadcasted_iota(jnp.int32, (1, half), 1)
    own[0] = real
    own[1] = jnp.where(bins == 0, 0.0, imag)
    own[2] = jnp.where(bins == 0, imag, real)

    tables[1].wait()
    if blocks == 1:
        for k in range(deep):
            unpack(slot_of(my_xy, k))

    def take(k):
        slot = slot_of(beside(k % (plane - 1)), partner(my_z, deep, k // (plane - 1)))
        arrived(slot)
        if blocks == 1:
            unpack(slot)

    lax.fori_loop(0, (plane - 1) * deep, lambda k, carry: (take(k), carry)[1], 0)

    stride = comps * chunks

    def result(b):
        return pltpu.make_async_remote_copy(
            src_ref=outgoing.at[b],
            dst_ref=incoming.at[b],
            send_sem=result_sem.at[b],
            recv_sem=result_sem.at[blocks + b],
            device_id=place(my_xy, my_z, other),
            device_id_type=MESH,
        )

    def compare(b):
        if blocks > 1:
            flat[...] = (
                gathered[pl.ds(b * block, block)]
                .astype(jnp.float32)
                .reshape(block * n * comps * chunks, LANES)
            )
        for c in range(comps):
            for q in range(chunks):
                waves[c * rows_block : (c + 1) * rows_block, q * LANES : (q + 1) * LANES] = flat[
                    pl.ds(c * chunks + q, rows_block, stride=stride), :
                ].astype(jnp.bfloat16)

        def multiply(core, f):
            g = half + f
            for j in range(0, rows_block, 16):
                for i in range(core * n, (core + 1) * n):
                    even, odd = 0.0, 0.0
                    for c in range(comps):
                        at = c * rows_block + j
                        real = spectra[at : at + 16, f : f + LANES]
                        imag = spectra[at : at + 16, g : g + LANES]
                        r = i * comps + c
                        plain = own[0, r : r + 1, f : f + LANES]
                        turned = own[1, r : r + 1, f : f + LANES]
                        mixed = own[2, r : r + 1, f : f + LANES]
                        even = even + (plain * real + turned * imag)
                        odd = odd + (mixed * imag - turned * real)
                    at = i * rows_block + j
                    cross[at : at + 16, f : f + LANES] = even.astype(jnp.bfloat16)
                    cross[at : at + 16, g : g + LANES] = odd.astype(jnp.bfloat16)

        for f in range(0, half, LANES):
            g = half + f
            basis = jnp.concatenate(
                [forward[:, f : f + LANES], forward[:, g : g + LANES]], axis=1
            )
            found = jnp.dot(waves[...], basis, preferred_element_type=jnp.float32)
            found = found.astype(jnp.bfloat16).astype(jnp.float32)
            spectra[:, f : f + LANES] = found[:, :LANES]
            spectra[:, g : g + LANES] = found[:, LANES:]
            multiply(1, f)

        def similar(core):
            if core == 0:
                for f in range(0, half, LANES):
                    multiply(0, f)
            first = core * n * rows_block
            lagged = jnp.dot(
                cross[first : first + n * rows_block],
                inverse[...],
                preferred_element_type=jnp.float32,
            )
            top = lagged[:, :LANES]
            for at in range(LANES, LAGS, LANES):
                top = jnp.maximum(top, lagged[:, at : at + LANES])
            flipped = jnp.max(top.T, axis=0, keepdims=True)
            return jnp.concatenate(
                [flipped[:, i * rows_block : (i + 1) * rows_block] for i in range(n)], axis=0
            )

        outgoing[b] = similar(1)
        result(b).start()
        out = similar(0)
        result(b).wait_recv()
        theirs = incoming[b]
        low = jnp.where(my_core == 0, out, theirs)
        high = jnp.where(my_core == 0, theirs, out)
        if blocks == 1:
            part = cols * n
            out_ref[...] = jnp.concatenate(
                [
                    kind[:, y * part : (y + 1) * part]
                    for y in range(tall)
                    for kind in (low, high)
                ],
                axis=1,
            )
        else:
            out_ref[b, 0] = low
            out_ref[b, 1] = high
        result(b).wait_send()

    each(blocks, compare)

    each(
        deep * (plane - 1),
        lambda k: to_plane(mine, k // (plane - 1), k % (plane - 1)).wait_send(),
    )
    each(deep - 1, lambda k: to_column(k).wait_send())
    to_sibling().wait_send()


def body(templates):
    n, comps, samples = templates.shape
    rows = lax.axis_size("row")
    cols = lax.axis_size("col")
    slots = rows * cols // CORES
    block = math.gcd(slots, 16)
    blocks = slots // block
    chunks = samples // LANES
    transform_len = samples + LAGS // 2
    forward = forward_table(samples, transform_len)
    inverse = inverse_table(transform_len, LAGS)
    vmem = pl.BlockSpec(memory_space=pltpu.VMEM)
    hbm = pl.BlockSpec(memory_space=pltpu.HBM)
    local = CORES * n * comps
    shape = (n, CORES * slots * n) if blocks == 1 else (blocks, CORES, n, block * n)
    out = pl.pallas_call(
        functools.partial(kernel, rows, cols),
        out_shape=pltpu.VMEM(shape, jnp.float32),
        in_specs=[hbm, hbm, hbm],
        out_specs=vmem,
        scratch_shapes=[
            pltpu.VMEM(templates.shape, jnp.float32),
            pltpu.VMEM((CORES * n * comps * chunks, LANES), jnp.float32),
            pltpu.VMEM((slots + 1, n * comps, chunks, LANES), jnp.bfloat16),
            pltpu.VMEM(forward.shape, jnp.bfloat16),
            pltpu.VMEM(inverse.shape, jnp.bfloat16),
            pltpu.VMEM((block * n * comps * chunks, LANES), jnp.float32),
            pltpu.VMEM((comps * block * n, samples), jnp.bfloat16),
            pltpu.VMEM((3, local + -local % 16, transform_len // 2), jnp.float32),
            pltpu.VMEM((comps * block * n, transform_len), jnp.float32),
            pltpu.VMEM((CORES * n * block * n, transform_len), jnp.bfloat16),
            pltpu.VMEM((blocks, n, block * n), jnp.float32),
            pltpu.VMEM((blocks, n, block * n), jnp.float32),
            pltpu.SemaphoreType.DMA((slots + cols + 1,)),
            pltpu.SemaphoreType.DMA((slots + 1,)),
            pltpu.SemaphoreType.DMA((3,)),
            pltpu.SemaphoreType.DMA((2 * blocks,)),
        ],
        compiler_params=pltpu.CompilerParams(collective_id=0, has_side_effects=True),
    )(templates, forward, inverse)
    if blocks == 1:
        return out
    out = out.transpose(2, 1, 0, 3).reshape(n, CORES, rows // CORES, cols * n)
    return out.transpose(0, 2, 1, 3).reshape(n, CORES * slots * n)


def solution(mesh):
    placed = (P(("row", "col"), None, None),)
    return jax.shard_map(
        body, mesh=mesh, in_specs=placed, out_specs=P(("row", "col"), None), check_vma=False
    )
```
